128 devices in a mesh: stn: 4 (over z), chan: 4 (over y_hi, core), tile: 8 (over x, y_lo).
Axes of the slice: x: 4, y: 4 (y_hi: 2, y_lo: 2; y = y_hi * 2 + y_lo), z: 4, core: 2. Of those that a mesh axis runs over, the one named last changes fastest.
Arguments:
- model_image: bfloat16 [32, 64, 2048], P('tile', 'stn'), may hold values from -0.0029296875 to 0.0029296875
- station_beams: float32 [2, 64, 1024], replicated, may hold values from -6 to 6
- subgrid_offsets: int32 [4, 512, 2], P('chan'), may hold values from -4096 to 4064
- subgrid_stations: int32 [512, 2], P(('stn', 'tile')), may hold values from 0 to 63, as said below
- visibility_uv: float32 [2, 512, 512], P(None, ('stn', 'tile'), 'chan'), may hold values from 2 to 30
- observed: float32 [2, 128, 4, 512], P(None, ('stn', 'tile'), 'chan'), may hold values from -3 to 3
- live_counts: int32 [128, 4], P(('stn', 'tile'), 'chan'), may hold values from 1 to 8
Outputs:
- residual: float32 [2, 128, 4, 512], P(None, ('stn', 'tile'), 'chan')
The draws below stay inside these ranges and needn't reach their ends.
Inputs may be any that keep to these rules, and one draw needn't show every extreme that they name: `subgrid_stations`: each row names two different stations. `live_counts`: rows with a time step at or beyond the count carry no data.
All inputs are finite; a program needn't handle non-finite values.
Results may differ from the reference program's by a relative error of at most 0.00071.
Values may be sent and summed in bfloat16 or wider, within the bound.
A program may use at most 64 MiB of HBM per device.

```python
import math
import jax
import jax.numpy as jnp
from jax import lax

SG = 32
NG = 8192
STATIONS = 64
CHAN_GRP = 16
TIMES = 8
TM = 2048
TL = 64
TILES = 32
VROWS = 512
NSUB = 512
N_CHAN = 4


def draw_subgrid_stations(key, part):
    station_key = jax.random.fold_in(key, 11)
    stride_key = jax.random.fold_in(key, 12)
    station_one = jax.random.randint(station_key, (NSUB,), 0, STATIONS, dtype=jnp.int32)
    stride = jax.random.randint(stride_key, (NSUB,), 1, STATIONS, dtype=jnp.int32)
    station_two = jnp.mod(station_one + stride, STATIONS)
    return jnp.stack([station_one, station_two], axis=1)


def with_ends(array, stream_key, smallest, high):
    longest = array.shape.index(max(array.shape))
    spots = []
    for shift in (0, 1):
        where = [jax.random.randint(jax.random.fold_in(stream_key, axis), (), 0, length) for axis, length in enumerate(array.shape)]
        where[longest] = (where[longest] + shift) % array.shape[longest]
        spots.append(tuple(where))
    return array.at[spots[0]].set(smallest).at[spots[1]].set(high)


def block_scale(key, dims, shards, low, high):
    loudness, own = 1.0, jax.random.fold_in(key, 6)
    for axis_at, parts in shards:
        steps = jnp.exp(jax.random.uniform(jax.random.fold_in(own, axis_at), (parts,), jnp.float32, low / len(shards), high / len(shards)))
        loudness = loudness * jnp.repeat(steps, dims[axis_at] // parts).reshape([-1 if axis == axis_at else 1 for axis in range(len(dims))])
    return loudness


def noise(own_key, extent, spread, most, pieces=(), kind=jnp.bfloat16):
    drawn = jax.random.normal(own_key, extent, jnp.float32) * spread
    if len(pieces) > 0:
        drawn = block_scale(own_key, extent, pieces, -0.22, 0.18) * drawn
    return jnp.clip(drawn, min=-most, max=most).astype(kind)


def setup_inputs(seed: int = 0) -> dict:
    splits = jax.random.split(jax.random.key(seed), 8)
    model_image = noise(splits[0], (TILES, TL, TM), (TILES * TL * TM) ** -0.5, 0.0029296875, ((0, 8), (1, 4)))
    station_beams = noise(splits[1], (2, STATIONS, SG * SG), 1.0, 6.0, (), jnp.float32)
    subgrid_offsets = with_ends(jax.random.randint(splits[2], (N_CHAN, NSUB, 2), 0 - NG // 2, NG // 2 - SG + 1), jax.random.fold_in(splits[2], 1), 0 - NG // 2, (NG // 2 - SG + 1) - 1).astype(jnp.int32)
    subgrid_stations = draw_subgrid_stations(jax.random.fold_in(splits[7], 71), 0)
    visibility_uv = jnp.clip(2.0 + 28.0 * jax.random.uniform(splits[4], (2, NSUB, VROWS), jnp.float32) ** block_scale(splits[4], (2, NSUB, VROWS), ((1, 32), (2, 4)), -0.2, 0.2), 2.0, 30.0)
    observed = noise(splits[5], (2, NSUB // N_CHAN, N_CHAN, VROWS), 0.5, 3.0, ((1, 32), (2, 4)), jnp.float32)
    live_counts = with_ends(jax.random.randint(splits[6], (NSUB // N_CHAN, N_CHAN), 1, TIMES + 1), jax.random.fold_in(splits[6], 1), 1, TIMES).astype(jnp.int32)
    return dict(model_image=model_image, station_beams=station_beams, subgrid_offsets=subgrid_offsets, subgrid_stations=subgrid_stations, visibility_uv=visibility_uv, observed=observed, live_counts=live_counts)


two_pi = 6.283185307179586


def phase_pair(products, modulus):
    angle_turns = jnp.mod(products, modulus).astype(jnp.float32) * (two_pi / modulus)
    return jnp.cos(angle_turns), -jnp.sin(angle_turns)


def contract(pattern, left, right):
    return jnp.einsum(pattern, left.astype(jnp.float32), right.astype(jnp.float32), precision=lax.Precision.HIGHEST)


def tile_cuts(strip_rows, row_ids, offset_block, strip_half):
    block_size = offset_block.shape[0]
    columns = strip_rows.shape[1]
    pixel_idx = jnp.arange(SG, dtype=jnp.int32)
    col_pos = jnp.arange(columns, dtype=jnp.int32) - columns // 2
    v_index = offset_block[:, 1][:, None] + pixel_idx[None, :]
    ev_real, ev_imag = phase_pair(col_pos[:, None, None] * v_index[None, :, :], NG)
    phase_table = jnp.stack([ev_real, ev_imag], axis=1).reshape(columns, 2 * block_size * SG).astype(jnp.bfloat16)
    partial_q = jnp.dot(strip_rows, phase_table, preferred_element_type=jnp.float32).astype(jnp.bfloat16)
    partial_q = partial_q.reshape(strip_rows.shape[0], 2, block_size, SG)
    q_real = partial_q[:, 0]
    q_imag = partial_q[:, 1]
    u_index = offset_block[:, 0][:, None] + pixel_idx[None, :]
    row_pos = (row_ids - strip_half).astype(jnp.int32)
    eu_real, eu_imag = phase_pair(u_index[:, :, None] * row_pos[None, None, :], NG)
    eu_real = eu_real.astype(jnp.bfloat16)
    eu_imag = eu_imag.astype(jnp.bfloat16)
    cut_real = contract("jal,ljb->jab", eu_real, q_real) - contract("jal,ljb->jab", eu_imag, q_imag)
    cut_imag = contract("jal,ljb->jab", eu_real, q_imag) + contract("jal,ljb->jab", eu_imag, q_real)
    return jnp.stack([cut_real, cut_imag], axis=1).reshape(block_size, 2 * SG * SG)


def cuts_blocked(strip_rows, row_ids, offsets, strip_half):
    how_many = offsets.shape[0]
    block_size = math.gcd(how_many, 32)
    grouped = offsets.reshape(how_many // block_size, block_size, 2)
    stacked = lax.map(lambda offset_block: tile_cuts(strip_rows, row_ids, offset_block, strip_half), grouped)
    return stacked.reshape(how_many, 2 * SG * SG)


def predict(cut_rows, pair_ids, station_beams, uv_block):
    how_many = cut_rows.shape[0]
    cut_grid = cut_rows.reshape(how_many, 2, SG, SG)
    pixel_idx = jnp.arange(SG, dtype=jnp.int32)
    w_real, w_neg = phase_pair(pixel_idx[:, None] * pixel_idx[None, :], SG)
    w_imag = -w_neg
    c_real = cut_grid[:, 0]
    c_imag = cut_grid[:, 1]
    half_real = contract("xa,jab->jxb", w_real, c_real) - contract("xa,jab->jxb", w_imag, c_imag)
    half_imag = contract("xa,jab->jxb", w_real, c_imag) + contract("xa,jab->jxb", w_imag, c_real)
    sub_real = (contract("jxb,yb->jxy", half_real, w_real) - contract("jxb,yb->jxy", half_imag, w_imag)) / (SG * SG)
    sub_imag = (contract("jxb,yb->jxy", half_real, w_imag) + contract("jxb,yb->jxy", half_imag, w_real)) / (SG * SG)
    pixel_pos = pixel_idx.astype(jnp.float32)
    taper_line = 1.0 - ((2.0 * pixel_pos - (SG - 1)) / SG) ** 2
    taper_grid = (taper_line[:, None] * taper_line[None, :]).reshape(SG * SG)
    beam_first = station_beams[:, pair_ids[:, 0]]
    beam_second = station_beams[:, pair_ids[:, 1]]
    gain_real = (beam_first[0] * beam_second[0] + beam_first[1] * beam_second[1]) * taper_grid
    gain_imag = (beam_first[1] * beam_second[0] - beam_first[0] * beam_second[1]) * taper_grid
    flat_real = sub_real.reshape(how_many, SG * SG)
    flat_imag = sub_imag.reshape(how_many, SG * SG)
    weighted_real = (flat_real * gain_real - flat_imag * gain_imag).reshape(how_many, SG, SG)
    weighted_imag = (flat_real * gain_imag + flat_imag * gain_real).reshape(how_many, SG, SG)
    u_angle = uv_block[0][:, :, None] * pixel_pos[None, None, :] * (two_pi / SG)
    v_angle = uv_block[1][:, :, None] * pixel_pos[None, None, :] * (two_pi / SG)
    eu_real = jnp.cos(u_angle)
    eu_imag = -jnp.sin(u_angle)
    ev_real = jnp.cos(v_angle)
    ev_imag = -jnp.sin(v_angle)
    inner_real = contract("jxy,jky->jxk", weighted_real, ev_real) - contract("jxy,jky->jxk", weighted_imag, ev_imag)
    inner_imag = contract("jxy,jky->jxk", weighted_real, ev_imag) + contract("jxy,jky->jxk", weighted_imag, ev_real)
    vis_real = contract("jkx,jxk->jk", eu_real, inner_real) - contract("jkx,jxk->jk", eu_imag, inner_imag)
    vis_imag = contract("jkx,jxk->jk", eu_real, inner_imag) + contract("jkx,jxk->jk", eu_imag, inner_real)
    return jnp.stack([vis_real, vis_imag], axis=0)


def reference(model_image, station_beams, subgrid_offsets, subgrid_stations, visibility_uv, observed, live_counts):
    strip_rows = model_image.reshape(TILES * TL, TM)
    row_ids = jnp.arange(TILES * TL, dtype=jnp.int32)
    strip_half = TILES * TL // 2
    vis_width = CHAN_GRP * TIMES
    predicted_parts = []
    for channel_group in range(N_CHAN):
        cut_rows = cuts_blocked(strip_rows, row_ids, subgrid_offsets[channel_group], strip_half)
        uv_block = visibility_uv[:, :, channel_group * vis_width:(channel_group + 1) * vis_width]
        predicted_parts.append(predict(cut_rows, subgrid_stations, station_beams, uv_block))
    predicted = jnp.concatenate(predicted_parts, axis=2).reshape(2, NSUB // N_CHAN, N_CHAN, VROWS)
    time_step = jnp.mod(jnp.arange(VROWS, dtype=jnp.int32), TIMES)
    live_mask = time_step[None, None, :] < live_counts[:, :, None]
    return jnp.where(live_mask[None], observed - predicted, 0.0)
```

```python
import functools
import math

import jax
import jax.numpy as jnp
import numpy as np
from jax import lax
from jax.experimental import pallas as pl
from jax.experimental.pallas import tpu as pltpu
from jax.sharding import Mesh
from jax.sharding import PartitionSpec as P

SG = 32
TILE = ("tile_0", "tile_1")
STN_TILE = ("stn", "tile_0", "tile_1")
CHAN = ("chan_0", "chan_1")
MESH = pl.DeviceIdType.MESH
F32 = jnp.float32
BF16 = jnp.bfloat16
VB = 272
VM = pltpu.VMEM
HI = lax.Precision.HIGHEST


def poly(r):
    r2 = r * r
    s = r * (1.0 + r2 * (-1 / 6 + r2 * (1 / 120 + r2 * (-1 / 5040 + r2 * (1 / 362880)))))
    c = 1.0 + r2 * (-0.5 + r2 * (1 / 24 + r2 * (-1 / 720 + r2 * (1 / 40320))))
    return c, s


def turn(q, c, s):
    swap = (q & 1) == 1
    cs = jnp.where(swap, s, c)
    sn = jnp.where(swap, c, s)
    cs = jnp.where(((q + 1) & 2) != 0, -cs, cs)
    sn = jnp.where((q & 2) != 0, -sn, sn)
    return cs, sn


def circle(p):
    p = p & 8191
    q = (p + 1024) >> 11
    c, s = poly((p - (q << 11)).astype(F32) * (2 * math.pi / 8192))
    return turn(q, c, s)


def circle_f(t):
    f = (t - jnp.floor(t)) * 4.0
    q = jnp.floor(f + 0.5)
    c, s = poly((f - q) * (math.pi / 2))
    return turn(q.astype(jnp.int32), c, s)


def iota(shape, dim):
    return lax.broadcasted_iota(jnp.int32, shape, dim)


def y_next(step):
    y = lax.rem(lax.axis_index("chan_0") * 2 + lax.axis_index("tile_1") + step + 4, 4)
    return {"chan_0": y // 2, "tile_1": lax.rem(y, 2)}


def gather_kernel(blk, off, img, offs, send, recv, osem):
    x = lax.axis_index("tile_0")
    c = lax.axis_index("chan_1")
    xp, xm, xo = lax.rem(x + 1, 4), lax.rem(x + 3, 4), lax.rem(x + 2, 4)
    yp, ym = y_next(1), y_next(-1)
    up, down = {"tile_0": xp}, {"tile_0": xm}
    bar = pltpu.get_barrier_semaphore()
    for d in (up, down, yp, ym, {"chan_1": 1 - c}):
        pl.semaphore_signal(bar, inc=1, device_id=d, device_id_type=MESH)
    pl.semaphore_wait(bar, 5)
    offs[pl.ds(c, 1)] = off[...]
    oc = pltpu.make_async_remote_copy(
        off, offs.at[pl.ds(c, 1)], osem.at[0], osem.at[1], device_id={"chan_1": 1 - c}, device_id_type=MESH
    )
    oc.start()
    native = c == lax.axis_index("tile_1")

    def half(b, h):
        return img.at[b, pl.ds(h * 32, 32)]

    def copy(src, b, h, k, dev):
        return pltpu.make_async_remote_copy(
            src, half(b, h), send.at[k], recv.at[b, h], device_id=dev, device_id_type=MESH
        )

    def landed(b, h):
        pltpu.make_async_remote_copy(
            half(b, h), half(b, h), send.at[0], recv.at[b, h], device_id=up, device_id_type=MESH
        ).wait_recv()

    @pl.when(native)
    def _():
        own = [blk.at[pl.ds(h * 32, 32)] for h in range(2)]
        cs = [
            copy(own[0], x, 0, 0, up),
            copy(own[1], x, 1, 1, down),
            copy(own[0], x, 0, 2, ym),
            copy(own[1], x, 1, 3, yp),
            copy(own[1], x, 1, 4, up),
            copy(own[0], x, 0, 5, down),
        ]
        for k in cs:
            k.start()
        img[pl.ds(x, 1)] = blk[...][None]
        k = 6
        for b, h, relay in (
            (xm, 0, up),
            (xp, 1, down),
            (xm, 1, None),
            (xp, 0, None),
            (xo, 0, None),
            (xo, 1, None),
        ):
            landed(b, h)
            if relay is not None:
                cs.append(copy(half(b, h), b, h, k, relay))
                cs[-1].start()
                k += 1
            cs.append(copy(half(b, h), b, h, k, yp if h else ym))
            cs[-1].start()
            k += 1
        for q in cs:
            q.wait_send()

    @pl.when(jnp.logical_not(native))
    def _():
        for b in (x, xm, xp, xo):
            for h in range(2):
                landed(b, h)

    oc.wait()


def spectra(c_img, perm_t, etab, sbuf, qtab):
    for g in range(2):
        rows = c_img[pl.ds(2 * g, 2)].reshape(128, 2048)
        for q in range(4):
            o = lax.dot_general(
                perm_t[...], rows[:, q * 512 : q * 512 + 512], (((1,), (1,)), ((), ())), preferred_element_type=F32
            ).astype(BF16)
            for s in range(4):
                sbuf[pl.ds(s * 512 + q * 128, 128), pl.ds(g * 128, 128)] = o[s * 128 : s * 128 + 128]


def phase_table(etab):
    def column(lc, _):
        lane = iota((16, 128), 1)
        m = (lc & 3) * 512 + 4 * lane + (lc >> 2) - 1024
        bc, bs = circle(iota((16, 128), 0) * m)
        ar, ai = circle((iota((72, 128), 0) * 16 - 32) * m[:1])
        at = pl.ds(pl.multiple_of(lc * 128, 128), 128)
        for t in range(68):
            r, i = ar[t : t + 1], ai[t : t + 1]
            n, w = divmod(t, 17)
            etab[n, 0, pl.ds(w * 16, 16), at] = (r * bc - i * bs).astype(BF16)
            etab[n, 1, pl.ds(w * 16, 16), at] = -(r * bs + i * bc).astype(BF16)
        return 0

    lax.fori_loop(0, 16, column, 0)


def q_stage(img_t, etab, sums, qtab):
    def block(n, _):
        for s in range(4):
            e = etab[n, :, :, pl.ds(s * 512, 512)].reshape(2 * VB, 512)
            o = jnp.dot(e, img_t[pl.ds(s * 512, 512)], preferred_element_type=F32)
            sums[s] = o.reshape(2, VB, 256)
        for w in range(VB // 16):
            at = pl.ds(w * 16, 16)
            re = [sums[s, 0, at] for s in range(4)]
            im = [sums[s, 1, at] for s in range(4)]
            ar, ai, br, bi = re[0] + re[2], im[0] + im[2], re[0] - re[2], im[0] - im[2]
            cr, ci, dr, di = re[1] + re[3], im[1] + im[3], re[1] - re[3], im[1] - im[3]
            outs = ((ar + cr, ai + ci), (br + di, bi - dr), (ar - cr, ai - ci), (br - di, bi + dr))
            to = pl.ds(pl.multiple_of(n * VB + w * 16, 16), 16)
            for k in range(4):
                for p in range(2):
                    for h in range(2):
                        qtab[k, p, h, to] = outs[k][p][:, h * 128 : h * 128 + 128]
        return 0

    lax.fori_loop(0, 4, block, 0)


def place(v0):
    w0 = v0 & 8191
    kq, rm = w0 >> 11, w0 & 2047
    fwd = rm <= 1024
    k = jnp.where(fwd, kq, (3 - kq) & 3)
    start = jnp.where(fwd, rm + 32, 2049 - rm)
    sign = jnp.where(fwd, 1.0, -1.0).astype(F32)
    return k, start, sign


def row_pos(shape, dim, c, z):
    r = iota(shape, dim)
    return ((((r >> 6) * 2 + c) * 4 + ((r >> 4) & 3)) * 64 + z * 16 + (r & 15)) - 1024


def eu_tables(offs_v, ztab, eab, c, z):
    l1 = row_pos((1, 256), 1, c, z)
    ec, es = circle(iota((32, 256), 0) * l1)
    eab[0] = ec
    eab[1] = es
    eye = iota((64, 128), 0) == iota((64, 128), 1)
    for k in range(2):
        u = jnp.broadcast_to(offs_v[k : k + 1].astype(F32), (64, 128))
        u = jnp.sum(jnp.where(eye, u, 0.0), axis=1, keepdims=True).astype(jnp.int32)
        zc, zs = circle(u * l1)
        ztab[0, pl.ds(k * 64, 64)] = zc
        ztab[1, pl.ds(k * 64, 64)] = zs


def cut_stage(offs_s, ztab, eab, qtab, cuts):
    lane = iota((32, 128), 1)
    first = (lane & 63) < 32
    low = lane < 64

    def pair(t, _):
        left, res, ims = [], [], []
        core, i = t // 32, lax.rem(t, 32) * 2
        for e in range(2):
            j = t * 2 + e
            k, start, sign = place(offs_s[core, 64 + i + e])
            zc, zs = ztab[0, pl.ds(j, 1)], ztab[1, pl.ds(j, 1)]
            ec, es = eab[0], eab[1]
            left.append((zc * ec - zs * es).astype(BF16))
            left.append(-(zc * es + zs * ec).astype(BF16))
            at = pl.ds(start, 32)
            res.append(jnp.concatenate([qtab[k, 0, h, at] for h in range(2)], axis=1).astype(BF16))
            ims.append((jnp.concatenate([qtab[k, 1, h, at] for h in range(2)], axis=1) * sign).astype(BF16))
        o = lax.dot_general(
            jnp.concatenate(left, axis=0),
            jnp.concatenate(res + ims, axis=0),
            (((1,), (1,)), ((), ())),
            preferred_element_type=F32,
        )
        a = jnp.where(first, o[0:32], o[64:96])
        b = pltpu.roll(jnp.where(first, o[32:64], o[96:128]), 64, 1)
        cuts[t] = jnp.where(low, a - b, a + b)
        return 0

    lax.fori_loop(0, 64, pair, 0, unroll=2)


def middle_kernel(img, perm_t, offs_v, offs_s, cuts, etab, img_t, sums, qtab, ztab, eab):
    c, z = lax.axis_index("chan_1"), lax.axis_index("stn")
    phase_table(etab)
    eu_tables(offs_v, ztab, eab, c, z)
    spectra(img, perm_t, etab, img_t, qtab)
    q_stage(img_t, etab, sums, qtab)
    cut_stage(offs_s, ztab, eab, qtab, cuts)


def reduce_kernel(cuts, out, mine, dbuf, hbuf, rbuf, dsend, drecv, hsend, hrecv, rsend, rrecv):
    z = lax.axis_index("stn")
    c = lax.axis_index("chan_1")
    zp, zm, zo = lax.rem(z + 1, 4), lax.rem(z + 3, 4), lax.rem(z + 2, 4)
    up, down, twin = {"stn": zp}, {"stn": zm}, {"chan_1": 1 - c}
    bar = pltpu.get_barrier_semaphore()
    for d in (up, down, twin):
        pl.semaphore_signal(bar, inc=1, device_id=d, device_id_type=MESH)
    pl.semaphore_wait(bar, 3)

    def rc(src, dst, s, r, dev):
        return pltpu.make_async_remote_copy(src, dst, s, r, device_id=dev, device_id_type=MESH)

    d = [rc(cuts.at[1 - c, q], dbuf.at[q], dsend.at[q], drecv.at[q], twin) for q in (zo, zp, zm, z)]
    for q in d:
        q.start()
    lo, hi = pl.ds(0, 4), pl.ds(4, 4)
    d[0].wait_recv()
    mine[0] = cuts[c, zo] + dbuf[zo]
    h = [
        rc(mine.at[0, lo], hbuf.at[0], hsend.at[0], hrecv.at[0], up),
        rc(mine.at[0, hi], hbuf.at[1], hsend.at[1], hrecv.at[1], down),
    ]
    for q in h:
        q.start()
    d[1].wait_recv()
    mine[1] = cuts[c, zp] + dbuf[zp]
    r = [
        rc(mine.at[1, lo], rbuf.at[0, lo], rsend.at[0], rrecv.at[0], up),
        rc(mine.at[1, hi], rbuf.at[0, hi], rsend.at[1], rrecv.at[1], up),
        rc(mine.at[2, lo], rbuf.at[1, lo], rsend.at[2], rrecv.at[2], down),
        rc(mine.at[2, hi], rbuf.at[1, hi], rsend.at[3], rrecv.at[3], down),
    ]
    r[1].start()
    d[2].wait_recv()
    mine[2] = cuts[c, zm] + dbuf[zm]
    r[2].start()
    d[3].wait_recv()
    mine[3] = cuts[c, z] + dbuf[z]
    h[0].wait_recv()
    mine[1, lo] = mine[1, lo] + hbuf[0]
    r[0].start()
    h[1].wait_recv()
    mine[2, hi] = mine[2, hi] + hbuf[1]
    r[3].start()
    for q in r:
        q.wait_recv()
    out[...] = mine[3] + rbuf[0] + rbuf[1]
    for q in d + h + r:
        q.wait_send()


def dft_tables(mtab, tabs):
    row, col = iota((128, 512), 0), iota((128, 512), 1)
    b, y = row & 31, col & 31
    cs, sn = circle(((b * y) & 31) * 256)
    same = ((row >> 5) & 1) == (col >> 8)
    rim, cim = row >> 6, (col >> 7) & 1
    v = jnp.where(rim == cim, cs, jnp.where(rim == 1, -sn, sn))
    mtab[...] = jnp.where(same, v, 0.0)
    a, l2 = iota((32, 128), 0), iota((32, 128), 1)
    s, y2 = l2 >> 5, l2 & 31
    for f in range(2):
        p = a * s if f == 0 else y2 - a * s
        tc, ts = circle((p & 31) * 256)
        tabs[f, 0] = tc
        tabs[f, 1] = ts


def predict_body(cut, mtab, tabs, vs, v_at, ids, beams, uv, put):
    lane = iota((32, 128), 1)
    stacked = []
    flags = []
    for p in range(8):
        sg = [place(vs(2 * p + e))[2] for e in range(2)]
        flags += sg
        odd = (lane & 32) != 0
        sv = jnp.where(odd, jnp.full((32, 128), sg[1]), jnp.full((32, 128), sg[0]))
        x = cut(p)
        stacked.append(jnp.where(lane < 64, x, x * sv))
    t = jnp.dot(jnp.concatenate(stacked, axis=0), mtab[...], precision=HI, preferred_element_type=F32)
    fold = []
    for j in range(16):
        p, e = divmod(j, 2)
        tr = t[32 * p : 32 * p + 32, 256 * e : 256 * e + 128]
        ti = t[32 * p : 32 * p + 32, 256 * e + 128 : 256 * e + 256]
        fwd = jnp.full((32, 128), flags[j]) > 0.0
        wr = jnp.where(fwd, tabs[0, 0], tabs[1, 0])
        wi = jnp.where(fwd, tabs[0, 1], tabs[1, 1])
        r, i = tr * wr - ti * wi, (tr * wi + ti * wr) * flags[j]
        fold.append(r[0:8] + r[8:16] + r[16:24] + r[24:32])
        fold.append(i[0:8] + i[8:16] + i[16:24] + i[24:32])
    k16, a8 = iota((16, 8), 0), iota((16, 8), 1)
    cc, ss = circle((((k16 & 7) * a8) & 7) * 1024)
    f8 = jnp.where(k16 < 8, cc, ss)
    sub = jnp.dot(f8, jnp.concatenate(fold, axis=1), precision=HI, preferred_element_type=F32)
    t8, l8 = iota((8, 128), 0), iota((8, 128), 1)
    xx, yy = (t8 * 4 + (l8 >> 5)).astype(F32), (l8 & 31).astype(F32)
    tx, ty = (2.0 * xx - 31.0) / 32.0, (2.0 * yy - 31.0) / 32.0
    taper = (1.0 - tx * tx) * (1.0 - ty * ty) * (1.0 / 1024)
    t8f = t8.astype(F32)
    for j in range(16):
        at = 256 * j
        sr = sub[0:8, at : at + 128] - sub[8:16, at + 128 : at + 256]
        si = sub[0:8, at + 128 : at + 256] + sub[8:16, at : at + 128]
        ip, iq = ids(j)
        pr, pi, qr, qi = beams[0, ip], beams[1, ip], beams[0, iq], beams[1, iq]
        gr, gi = (pr * qr + pi * qi) * taper, (pi * qr - pr * qi) * taper
        wr, wi = sr * gr - si * gi, sr * gi + si * gr
        rows = [jnp.where((l8 >> 5) == s, w, 0.0) for w in (wr, wi) for s in range(4)]
        du, dv = uv[0, j : j + 1], uv[1, j : j + 1]
        vc, vsn = circle_f(dv * (1 / 32) * t8f)
        evr, evi = [], []
        for g in range(4):
            if g == 0:
                r, i = vc, -vsn
            else:
                gc, gs = circle_f(dv * (g / 4))
                r, i = vc * gc - vsn * gs, -(vc * gs + vsn * gc)
            evr.append(r)
            evi.append(i)
        er, ei = jnp.concatenate(evr, axis=0), jnp.concatenate(evi, axis=0)
        right = jnp.concatenate([jnp.concatenate([er] * 4, axis=0), jnp.concatenate([ei] * 4, axis=0)], axis=1)
        o = jnp.dot(jnp.concatenate(rows, axis=0), right, precision=HI, preferred_element_type=F32)
        nr = o[:32, :128] - o[32:, 128:]
        ni = o[:32, 128:] + o[32:, :128]
        uc, us = circle_f(du * (1 / 8) * t8f)
        vr = vi = 0.0
        for s in range(4):
            if s == 0:
                r, i = uc, -us
            else:
                sc, sn = circle_f(du * (s / 32))
                r, i = uc * sc - us * sn, -(uc * sn + us * sc)
            a, b = nr[8 * s : 8 * s + 8], ni[8 * s : 8 * s + 8]
            vr = vr + (r * a - i * b)
            vi = vi + (r * b + i * a)
        put(j, jnp.sum(vr, axis=0, keepdims=True), jnp.sum(vi, axis=0, keepdims=True))


def predict_kernel(cut, offs_s, ids, beams, uv, out, mtab, tabs):
    dft_tables(mtab, tabs)
    c, z = lax.axis_index("chan_1"), lax.axis_index("stn")

    def put(j, re, im):
        out[j % 4, pl.ds(j // 4, 1)] = re
        out[j % 4, pl.ds(4 + j // 4, 1)] = im

    predict_body(
        lambda p: cut[p],
        mtab,
        tabs,
        lambda j: offs_s[c, 64 + z * 16 + j],
        None,
        lambda j: (ids[j, 0], ids[j, 1]),
        beams,
        uv,
        put,
    )


def regroup_kernel(pred, obs, live, out, got, send, recv):
    h, c = lax.axis_index("chan_0"), lax.axis_index("chan_1")
    me = h * 2 + c
    others = [(h, 1 - c), (1 - h, c), (1 - h, 1 - c)]
    devs = [{"chan_0": a, "chan_1": b} for a, b in others]
    bar = pltpu.get_barrier_semaphore()
    for d in devs:
        pl.semaphore_signal(bar, inc=1, device_id=d, device_id_type=MESH)
    pl.semaphore_wait(bar, 3)
    cs = []
    for n, (a, b) in enumerate(others):
        cs.append(
            pltpu.make_async_remote_copy(
                pred.at[a * 2 + b], got.at[me], send.at[n], recv.at[n], device_id=devs[n], device_id_type=MESH
            )
        )
        cs[-1].start()
    got[me] = pred[me]
    for q in cs:
        q.wait_recv()
    row, lane = iota((8, 128), 0) & 3, iota((8, 128), 1)
    count = jnp.zeros((8, 128), jnp.int32)
    for p in range(4):
        count = jnp.where(row == p, jnp.full((8, 128), live[p, 0]), count)
    keep = (lane & 7) < count
    for s in range(4):
        at = pl.ds(s * 128, 128)
        out[:, at] = jnp.where(keep, obs[:, at] - got[s], 0.0)
    for q in cs:
        q.wait_send()


def spec(n, smem=()):
    return [pl.BlockSpec(memory_space=pltpu.SMEM if i in smem else VM) for i in range(n)]


def params(cid=None, vmem=None):
    kw = {}
    if cid is not None:
        kw = dict(collective_id=cid, has_side_effects=True)
    return pltpu.CompilerParams(vmem_limit_bytes=vmem, **kw)


def on_device(image, beams, offsets, stations, uv, observed, live):
    perm = np.zeros((512, 512), np.float32)
    for s in range(4):
        perm[s * 128 + np.arange(128), 4 * np.arange(128) + s] = 1
    perm_t = jnp.asarray(perm, BF16)
    tile = lax.axis_index(TILE)
    mine = lax.dynamic_index_in_dim(offsets.reshape(4, 8, 16, 2), tile, 1, keepdims=False)
    off = mine.reshape(64, 2).T.reshape(1, 128)
    dma = pltpu.SemaphoreType.DMA
    sd = jax.ShapeDtypeStruct
    img, offs = pl.pallas_call(
        gather_kernel,
        name="gather",
        out_shape=(sd((4, 64, 2048), BF16), sd((2, 128), jnp.int32)),
        in_specs=spec(2),
        out_specs=tuple(spec(2)),
        scratch_shapes=[dma((14,)), dma((4, 2)), dma((2,))],
        compiler_params=params(0),
    )(image.reshape(64, 2048), off)
    cuts = pl.pallas_call(
        middle_kernel,
        name="middle",
        out_shape=sd((64, 32, 128), F32),
        in_specs=spec(4, (3,)),
        out_specs=spec(1)[0],
        scratch_shapes=[
            VM((4, 2, VB, 2048), BF16),
            VM((2048, 256), BF16),
            VM((4, 2, VB, 256), F32),
            VM((4, 2, 2, 4 * VB, 128), F32),
            VM((2, 128, 256), F32),
            VM((2, 32, 256), F32),
        ],
        compiler_params=params(None, 48 << 20),
    )(img, perm_t, offs, offs)
    cut = pl.pallas_call(
        reduce_kernel,
        name="reduce",
        out_shape=sd((8, 32, 128), F32),
        in_specs=spec(1),
        out_specs=spec(1)[0],
        scratch_shapes=[
            VM((4, 8, 32, 128), F32),
            VM((4, 8, 32, 128), F32),
            VM((2, 4, 32, 128), F32),
            VM((2, 8, 32, 128), F32),
            dma((4,)),
            dma((4,)),
            dma((2,)),
            dma((2,)),
            dma((4,)),
            dma((4,)),
        ],
        compiler_params=params(1),
    )(cuts.reshape(2, 4, 8, 32, 128))
    pred = pl.pallas_call(
        predict_kernel,
        name="predict",
        out_shape=sd((4, 8, 128), F32),
        in_specs=spec(5, (1, 2)),
        out_specs=spec(1)[0],
        scratch_shapes=[VM((128, 512), F32), VM((2, 2, 32, 128), F32)],
        compiler_params=params(),
    )(cut, offs, stations, beams.reshape(2, 64, 8, 128), uv)
    out = pl.pallas_call(
        regroup_kernel,
        name="regroup",
        out_shape=sd((8, 512), F32),
        in_specs=spec(3, (2,)),
        out_specs=spec(1)[0],
        scratch_shapes=[VM((4, 8, 128), F32), dma((3,)), dma((3,))],
        compiler_params=params(2),
    )(pred, observed.reshape(8, 512), live)
    return out.reshape(2, 4, 1, 512)


def solution(mesh):
    finer = Mesh(
        mesh.devices.reshape(mesh.shape["stn"], 2, 2, 4, 2),
        ("stn", "chan_0", "chan_1", "tile_0", "tile_1"),
    )
    placed = (
        P(TILE, "stn", None),
        P(),
        P(CHAN, None, None),
        P(STN_TILE, None),
        P(None, STN_TILE, CHAN),
        P(None, STN_TILE, CHAN, None),
        P(STN_TILE, CHAN),
    )
    return jax.shard_map(
        on_device,
        mesh=finer,
        in_specs=placed,
        out_specs=P(None, STN_TILE, CHAN, None),
        check_vma=False,
    )
```

```python
import functools
import math

import jax
import jax.numpy as jnp
import numpy as np
from jax import lax
from jax.experimental import pallas as pl
from jax.experimental.pallas import tpu as pltpu
from jax.sharding import Mesh
from jax.sharding import PartitionSpec as P

SG = 32
TILE = ("tile_0", "tile_1")
STN_TILE = ("stn", "tile_0", "tile_1")
CHAN = ("chan_0", "chan_1")
MESH = pl.DeviceIdType.MESH
F32 = jnp.float32
BF16 = jnp.bfloat16
VB = 272
VM = pltpu.VMEM


def poly(r):
    r2 = r * r
    s = r * (1.0 + r2 * (-1 / 6 + r2 * (1 / 120 + r2 * (-1 / 5040 + r2 * (1 / 362880)))))
    c = 1.0 + r2 * (-0.5 + r2 * (1 / 24 + r2 * (-1 / 720 + r2 * (1 / 40320))))
    return c, s


def turn(q, c, s):
    swap = (q & 1) == 1
    cs = jnp.where(swap, s, c)
    sn = jnp.where(swap, c, s)
    cs = jnp.where(((q + 1) & 2) != 0, -cs, cs)
    sn = jnp.where((q & 2) != 0, -sn, sn)
    return cs, sn


def circle(p):
    p = p & 8191
    q = (p + 1024) >> 11
    c, s = poly((p - (q << 11)).astype(F32) * (2 * math.pi / 8192))
    return turn(q, c, s)


def circle_f(t):
    f = (t - jnp.floor(t)) * 4.0
    q = jnp.floor(f + 0.5)
    c, s = poly((f - q) * (math.pi / 2))
    return turn(q.astype(jnp.int32), c, s)


def iota(shape, dim):
    return lax.broadcasted_iota(jnp.int32, shape, dim)


def y_next(step):
    y = lax.rem(lax.axis_index("chan_0") * 2 + lax.axis_index("tile_1") + step + 4, 4)
    return {"chan_0": y // 2, "tile_1": lax.rem(y, 2)}


def remote(src, dst, send, recv, dev):
    return pltpu.make_async_remote_copy(src, dst, send, recv, device_id=dev, device_id_type=MESH)


def spectra(img, perm_t, img_t, g):
    rows = img[pl.ds(2 * g, 2)].reshape(128, 2048)
    for q in range(4):
        o = lax.dot_general(
            perm_t[...], rows[:, q * 512 : q * 512 + 512], (((1,), (1,)), ((), ())), preferred_element_type=F32
        ).astype(BF16)
        for s in range(4):
            img_t[pl.ds(s * 512 + q * 128, 128), pl.ds(g * 128, 128)] = o[s * 128 : s * 128 + 128]


def phase_table(etab, first, last):
    def column(lc, _):
        lane = iota((16, 128), 1)
        m = (lc & 3) * 512 + 4 * lane + (lc >> 2) - 1024
        bc, bs = circle(iota((16, 128), 0) * m)
        ar, ai = circle((iota((72, 128), 0) * 16 - 32) * m[:1])
        at = pl.ds(pl.multiple_of(lc * 128, 128), 128)
        for t in range(68):
            r, i = ar[t : t + 1], ai[t : t + 1]
            n, w = divmod(t, 17)
            etab[n, 0, pl.ds(w * 16, 16), at] = (r * bc - i * bs).astype(BF16)
            etab[n, 1, pl.ds(w * 16, 16), at] = -(r * bs + i * bc).astype(BF16)
        return 0

    lax.fori_loop(first, last, column, 0)


def q_stage(img_t, etab, sums, qtab):
    def block(n, _):
        for s in range(4):
            e = etab[n, :, :, pl.ds(s * 512, 512)].reshape(2 * VB, 512)
            o = jnp.dot(e, img_t[pl.ds(s * 512, 512)], preferred_element_type=F32)
            sums[s] = o.reshape(2, VB, 256)
        for w in range(VB // 16):
            at = pl.ds(w * 16, 16)
            re = [sums[s, 0, at] for s in range(4)]
            im = [sums[s, 1, at] for s in range(4)]
            ar, ai, br, bi = re[0] + re[2], im[0] + im[2], re[0] - re[2], im[0] - im[2]
            cr, ci, dr, di = re[1] + re[3], im[1] + im[3], re[1] - re[3], im[1] - im[3]
            outs = ((ar + cr, ai + ci), (br + di, bi - dr), (ar - cr, ai - ci), (br - di, bi + dr))
            to = pl.ds(pl.multiple_of(n * VB + w * 16, 16), 16)
            for k in range(4):
                for p in range(2):
                    for h in range(2):
                        qtab[k, p, h, to] = outs[k][p][:, h * 128 : h * 128 + 128]
        return 0

    lax.fori_loop(0, 4, block, 0)


def place(v0):
    w0 = v0 & 8191
    kq, rm = w0 >> 11, w0 & 2047
    fwd = rm <= 1024
    k = jnp.where(fwd, kq, (3 - kq) & 3)
    start = jnp.where(fwd, rm + 32, 2049 - rm)
    sign = jnp.where(fwd, 1.0, -1.0).astype(F32)
    return k, start, sign


def left_tables(offv, ztab, ltab, c, z, x, tile):
    r = iota((1, 256), 1)
    slot = r >> 6
    xx = (x + jnp.where(slot == 1, 3, jnp.where(slot == 2, 1, jnp.where(slot == 3, 2, 0)))) & 3
    l1 = (((xx * 2 + c) * 4 + ((r >> 4) & 3)) * 64 + z * 16 + (r & 15)) - 1024
    ec, es = circle(iota((32, 256), 0) * l1)
    j, col = iota((64, 512), 0), iota((64, 512), 1)
    eye = col == ((j >> 4) * 8 + tile) * 16 + (j & 15)
    for k in range(2):
        u = jnp.broadcast_to(offv[k, 0:1].astype(F32), (64, 512))
        u = jnp.sum(jnp.where(eye, u, 0.0), axis=1, keepdims=True).astype(jnp.int32)
        zc, zs = circle(u * l1)
        ztab[0, pl.ds(k * 64, 64)] = zc
        ztab[1, pl.ds(k * 64, 64)] = zs

    def group(t, _):
        core, zz, p = t // 32, lax.rem(t, 32) // 8, lax.rem(t, 8)
        for e in range(2):
            zc, zs = ztab[0, pl.ds(t * 2 + e, 1)], ztab[1, pl.ds(t * 2 + e, 1)]
            ltab[core, zz, p, pl.ds(64 * e, 32)] = (zc * ec - zs * es).astype(BF16)
            ltab[core, zz, p, pl.ds(64 * e + 32, 32)] = -(zc * es + zs * ec).astype(BF16)
        return 0

    lax.fori_loop(0, 64, group, 0, unroll=2)


def cut_chunk(offs, ltab, qtab, cuts, core, tile, pairs):
    lane = iota((32, 128), 1)
    first = (lane & 63) < 32
    low = lane < 64
    for zz, p in pairs:
        res, ims = [], []
        for e in range(2):
            k, start, sign = place(offs[core, 1, (zz * 8 + tile) * 16 + 2 * p + e])
            at = pl.ds(start, 32)
            res.append(jnp.concatenate([qtab[k, 0, h, at] for h in range(2)], axis=1).astype(BF16))
            ims.append((jnp.concatenate([qtab[k, 1, h, at] for h in range(2)], axis=1) * sign).astype(BF16))
        o = lax.dot_general(
            ltab[core, zz, p],
            jnp.concatenate(res + ims, axis=0),
            (((1,), (1,)), ((), ())),
            preferred_element_type=F32,
        )
        a = jnp.where(first, o[0:32], o[64:96])
        b = pltpu.roll(jnp.where(first, o[32:64], o[96:128]), 64, 1)
        cuts[core, zz, p] = jnp.where(low, a - b, a + b)


def dft_tables(mtab, tabs):
    row, col = iota((128, 512), 0), iota((128, 512), 1)
    b, y = row & 31, col & 31
    cs, sn = circle(((b * y) & 31) * 256)
    same = ((row >> 5) & 1) == (col >> 8)
    rim, cim = row >> 6, (col >> 7) & 1
    v = jnp.where(same, jnp.where(rim == cim, cs, jnp.where(rim == 1, -sn, sn)), 0.0)
    mtab[0] = v.astype(BF16)
    mtab[1] = (v - v.astype(BF16).astype(F32)).astype(BF16)
    a, l2 = iota((32, 128), 0), iota((32, 128), 1)
    s, y2 = l2 >> 5, l2 & 31
    for f in range(2):
        tc, ts = circle(((a * s if f == 0 else y2 - a * s) & 31) * 256)
        tabs[f, 0] = tc
        tabs[f, 1] = ts


def parts(v):
    hi = v.astype(BF16)
    return hi, (v - hi.astype(F32)).astype(BF16)


def dot3(left, hi, lo):
    a, b = parts(left)
    n = left.shape[0]
    o = jnp.dot(jnp.concatenate([a, b], axis=0), hi, preferred_element_type=F32)
    return o[:n] + o[n:] + jnp.dot(a, lo, preferred_element_type=F32)


def phasors(uv, beams, ids, evt, eut, gains):
    t8, l8 = iota((8, 128), 0), iota((8, 128), 1)
    xx, yy = (t8 * 4 + (l8 >> 5)).astype(F32), (l8 & 31).astype(F32)
    tx, ty = (2.0 * xx - 31.0) / 32.0, (2.0 * yy - 31.0) / 32.0
    taper = (1.0 - tx * tx) * (1.0 - ty * ty) * (1.0 / 1024)
    t8f = t8.astype(F32)

    def one(j, _):
        ip, iq = ids[0, j], ids[1, j]
        pr, pi, qr, qi = beams[0, ip], beams[1, ip], beams[0, iq], beams[1, iq]
        gains[j, 0] = (pr * qr + pi * qi) * taper
        gains[j, 1] = (pi * qr - pr * qi) * taper
        du, dv = uv[0, pl.ds(j, 1)], uv[1, pl.ds(j, 1)]
        vc, vsn = circle_f(dv * (1 / 32) * t8f)
        uc, us = circle_f(du * (1 / 8) * t8f)
        gc, gs = circle_f(dv * 0.25 * t8f)
        sc, sn = circle_f(du * (1 / 32) * t8f)
        for g in range(4):
            vr = vc * gc[g : g + 1] - vsn * gs[g : g + 1]
            vi = -(vc * gs[g : g + 1] + vsn * gc[g : g + 1])
            for p, w in enumerate((vr, vi)):
                hi, lo = parts(jnp.concatenate([w] * 2, axis=0))
                for k in range(4):
                    evt[j, 0, pl.ds(32 * k + 8 * g, 8), pl.ds(128 * p, 128)] = hi[:8]
                    evt[j, 1, pl.ds(32 * k + 8 * g, 8), pl.ds(128 * p, 128)] = lo[:8]
            eut[j, 0, pl.ds(8 * g, 8)] = uc * sc[g : g + 1] - us * sn[g : g + 1]
            eut[j, 1, pl.ds(8 * g, 8)] = -(uc * sn[g : g + 1] + us * sc[g : g + 1])
        return 0

    lax.fori_loop(0, 16, one, 0, unroll=2)


def predict(cut, sign, mtab, tabs, evt, eut, gains, pred):
    lane = iota((32, 128), 1)
    odd = (lane & 32) != 0
    stacked = []
    for p in range(8):
        sv = jnp.where(odd, jnp.full((32, 128), sign[2 * p + 1]), jnp.full((32, 128), sign[2 * p]))
        x = cut(p)
        stacked.append(jnp.where(lane < 64, x, x * sv))
    t = dot3(jnp.concatenate(stacked, axis=0), mtab[0], mtab[1])
    fold = []
    for j in range(16):
        p, e = divmod(j, 2)
        tr = t[32 * p : 32 * p + 32, 256 * e : 256 * e + 128]
        ti = t[32 * p : 32 * p + 32, 256 * e + 128 : 256 * e + 256]
        fwd = jnp.full((32, 128), sign[j]) > 0.0
        wr = jnp.where(fwd, tabs[0, 0], tabs[1, 0])
        wi = jnp.where(fwd, tabs[0, 1], tabs[1, 1])
        r, i = tr * wr - ti * wi, (tr * wi + ti * wr) * sign[j]
        fold.append(r[0:8] + r[8:16] + r[16:24] + r[24:32])
        fold.append(i[0:8] + i[8:16] + i[16:24] + i[24:32])
    k16, a8 = iota((16, 8), 0), iota((16, 8), 1)
    cc, ss = circle((((k16 & 7) * a8) & 7) * 1024)
    f8 = jnp.where(k16 < 8, cc, ss)
    hi, lo = parts(jnp.concatenate(fold, axis=1))
    sub = dot3(f8, hi, lo)
    l8 = iota((8, 128), 1)
    for j in range(16):
        at = 256 * j
        sr = sub[0:8, at : at + 128] - sub[8:16, at + 128 : at + 256]
        si = sub[0:8, at + 128 : at + 256] + sub[8:16, at : at + 128]
        gr, gi = gains[j, 0], gains[j, 1]
        wr, wi = sr * gr - si * gi, sr * gi + si * gr
        rows = [jnp.where((l8 >> 5) == s, w, 0.0) for w in (wr, wi) for s in range(4)]
        o = dot3(jnp.concatenate(rows, axis=0), evt[j, 0], evt[j, 1])
        nr = o[:32, :128] - o[32:, 128:]
        ni = o[:32, 128:] + o[32:, :128]
        er, ei = eut[j, 0], eut[j, 1]
        vr, vi = er * nr - ei * ni, er * ni + ei * nr
        pred[j % 4, pl.ds(j // 4, 1)] = jnp.sum(vr, axis=0, keepdims=True)
        pred[j % 4, pl.ds(4 + j // 4, 1)] = jnp.sum(vi, axis=0, keepdims=True)


def kernel(
    image, beams_h, offt, idst, uv_h, obs_h, livet, perm_h, out,
    img, img_t, offv, offs, beams, uv, obs, perm_t, ids, live,
    etab, sums, qtab, ztab, ltab, cuts, mine, dbuf, hbuf, rbuf,
    mtab, tabs, evt, eut, gains, pred, got,
    lsem, bsem, isend, irecv, osem, dsend, drecv, hsend, hrecv, rsend, rrecv, asend, arecv,
):
    z, h, c = lax.axis_index("stn"), lax.axis_index("chan_0"), lax.axis_index("chan_1")
    x, yl = lax.axis_index("tile_0"), lax.axis_index("tile_1")
    tile = x * 2 + yl
    local = pltpu.make_async_copy
    own_in = local(image, img.at[0], lsem.at[0])
    off_in = local(offt, offv.at[c], lsem.at[1])
    late = [
        local(perm_h, perm_t, lsem.at[2]),
        local(uv_h, uv, lsem.at[3]),
        local(obs_h, obs, lsem.at[4]),
        local(idst, ids, lsem.at[5]),
        local(livet, live, lsem.at[6]),
    ]
    late += [local(beams_h.at[:, :, pl.ds(128 * g, 128)], beams.at[:, :, g], bsem.at[g]) for g in range(8)]
    native = c == yl
    off_in.start()
    pl.when(native)(own_in.start)
    xp, xm = lax.rem(x + 1, 4), lax.rem(x + 3, 4)
    yp, ym = y_next(1), y_next(-1)
    up, down, twin = {"tile_0": xp}, {"tile_0": xm}, {"chan_1": 1 - c}
    zp, zm, zo = lax.rem(z + 1, 4), lax.rem(z + 3, 4), lax.rem(z + 2, 4)
    zup, zdown = {"stn": zp}, {"stn": zm}
    peers = [twin, {"chan_0": 1 - h}, {"chan_0": 1 - h, "chan_1": 1 - c}]
    bar = pltpu.get_barrier_semaphore()
    for d in (up, down, yp, ym, zup, zdown, *peers):
        pl.semaphore_signal(bar, inc=1, device_id=d, device_id_type=MESH)
    for q in late:
        q.start()
    pl.when(native)(own_in.wait)
    off_in.wait()
    pl.semaphore_wait(bar, 9)
    swap = remote(offv.at[c], offv.at[c], osem.at[0], osem.at[1], twin)
    swap.start()

    def half(b, k):
        return img.at[b, pl.ds(2 * k, 2)]

    def send(b, k, to, n, dev):
        return remote(half(b, k), half(to, k), isend.at[n], irecv.at[to, k], dev)

    first = [
        send(0, 0, 1, 0, up),
        send(0, 1, 2, 1, down),
        send(0, 0, 0, 2, ym),
        send(0, 1, 0, 3, yp),
        send(0, 1, 1, 4, up),
        send(0, 0, 2, 5, down),
    ]
    steps = [
        (1, 0, [send(1, 0, 3, 6, up), send(1, 0, 1, 7, ym)]),
        (2, 1, [send(2, 1, 3, 8, down), send(2, 1, 2, 9, yp)]),
        (1, 1, [send(1, 1, 1, 10, yp)]),
        (2, 0, [send(2, 0, 2, 11, ym)]),
        (3, 0, [send(3, 0, 3, 12, ym)]),
        (3, 1, [send(3, 1, 3, 13, yp)]),
    ]

    def landed(b, k):
        remote(half(b, k), half(b, k), isend.at[0], irecv.at[b, k], up).wait_recv()

    def forward(lo, hi):
        @pl.when(native)
        def _():
            for b, k, qs in steps[lo:hi]:
                landed(b, k)
                for q in qs:
                    q.start()

    @pl.when(native)
    def _():
        for q in first:
            q.start()

    phase_table(etab, 0, 8)
    forward(0, 2)
    phase_table(etab, 8, 12)
    forward(2, 4)
    phase_table(etab, 12, 16)
    forward(4, 6)
    swap.wait()
    tos = local(offv, offs, lsem.at[7])
    tos.start()
    left_tables(offv, ztab, ltab, c, z, x, tile)
    dft_tables(mtab, tabs)
    tos.wait()
    for q in late:
        q.wait()

    @pl.when(jnp.logical_not(native))
    def _():
        for b in range(4):
            for k in range(2):
                landed(b, k)

    for g in range(2):
        spectra(img, perm_t, img_t, g)
    q_stage(img_t, etab, sums, qtab)

    lo, hi, full = pl.ds(0, 4), pl.ds(4, 4), pl.ds(0, 8)
    early = [(zo, p) for p in range(8)] + [(zp, p) for p in range(4, 8)] + [(zm, p) for p in range(4)]
    rest = [(zp, p) for p in range(4)] + [(zm, p) for p in range(4, 8)] + [(z, p) for p in range(8)]
    ds = [
        remote(cuts.at[1 - c, zz, at], dbuf.at[s, at], dsend.at[n], drecv.at[n], twin)
        for n, (zz, s, at) in enumerate(
            ((zo, 0, full), (zp, 1, hi), (zm, 2, lo), (zp, 1, lo), (zm, 2, hi), (z, 3, full))
        )
    ]
    hs = [
        remote(mine.at[0, lo], hbuf.at[0], hsend.at[0], hrecv.at[0], zup),
        remote(mine.at[0, hi], hbuf.at[1], hsend.at[1], hrecv.at[1], zdown),
    ]
    rs = [
        remote(mine.at[1, lo], rbuf.at[0, lo], rsend.at[0], rrecv.at[0], zup),
        remote(mine.at[1, hi], rbuf.at[0, hi], rsend.at[1], rrecv.at[1], zup),
        remote(mine.at[2, lo], rbuf.at[1, lo], rsend.at[2], rrecv.at[2], zdown),
        remote(mine.at[2, hi], rbuf.at[1, hi], rsend.at[3], rrecv.at[3], zdown),
    ]
    cut_chunk(offs, ltab, qtab, cuts, 1 - c, tile, early)
    for q in ds[:3]:
        q.start()
    cut_chunk(offs, ltab, qtab, cuts, c, tile, early)
    ds[0].wait_recv()
    mine[0] = cuts[c, zo] + dbuf[0]
    for q in hs:
        q.start()
    ds[1].wait_recv()
    mine[1, hi] = cuts[c, zp, hi] + dbuf[1, hi]
    rs[1].start()
    ds[2].wait_recv()
    mine[2, lo] = cuts[c, zm, lo] + dbuf[2, lo]
    rs[2].start()
    cut_chunk(offs, ltab, qtab, cuts, 1 - c, tile, rest)
    for q in ds[3:]:
        q.start()
    cut_chunk(offs, ltab, qtab, cuts, c, tile, rest)
    ds[3].wait_recv()
    hs[0].wait_recv()
    mine[1, lo] = cuts[c, zp, lo] + dbuf[1, lo] + hbuf[0]
    rs[0].start()
    ds[4].wait_recv()
    hs[1].wait_recv()
    mine[2, hi] = cuts[c, zm, hi] + dbuf[2, hi] + hbuf[1]
    rs[3].start()
    ds[5].wait_recv()
    phasors(uv, beams, ids, evt, eut, gains)
    for q in rs:
        q.wait_recv()
    predict(
        lambda p: cuts[c, z, p] + dbuf[3, p] + rbuf[0, p] + rbuf[1, p],
        [place(offs[c, 1, (z * 8 + tile) * 16 + j])[2] for j in range(16)],
        mtab, tabs, evt, eut, gains, pred,
    )
    me = h * 2 + c
    other = [h * 2 + 1 - c, (1 - h) * 2 + c, (1 - h) * 2 + 1 - c]
    sends = [remote(pred.at[other[n]], got.at[me], asend.at[n], arecv.at[n], peers[n]) for n in range(3)]
    for q in sends:
        q.start()
    got[me] = pred[me]
    lane = iota((1, 128), 1)
    for q in sends:
        q.wait_recv()
    for p in range(4):
        keep = (lane & 7) < jnp.full((1, 128), live[0, p])
        for s in range(4):
            at = pl.ds(s * 128, 128)
            for r in range(2):
                out[r, p, :, at] = jnp.where(keep, obs[r, p, :, at] - got[s, pl.ds(4 * r + p, 1)], 0.0)

    @pl.when(native)
    def _():
        for q in first + [q for s in steps for q in s[2]]:
            q.wait_send()

    for q in ds + hs + rs + sends:
        q.wait_send()


def on_device(image, beams, offsets, stations, uv, observed, live):
    perm = np.zeros((512, 512), np.float32)
    for s in range(4):
        perm[s * 128 + np.arange(128), 4 * np.arange(128) + s] = 1
    dma = pltpu.SemaphoreType.DMA
    i32 = jnp.int32
    sm = pltpu.SMEM
    return pl.pallas_call(
        kernel,
        name="degrid",
        out_shape=jax.ShapeDtypeStruct((2, 4, 1, 512), F32),
        in_specs=[pl.BlockSpec(memory_space=pl.ANY)] * 8,
        out_specs=pl.BlockSpec(memory_space=VM),
        scratch_shapes=[
            VM((4, 4, 16, 2048), BF16),
            VM((2048, 256), BF16),
            VM((2, 2, 512), i32),
            sm((2, 2, 512), i32),
            VM((2, 64, 8, 128), F32),
            VM((2, 16, 128), F32),
            VM((2, 4, 1, 512), F32),
            VM((512, 512), BF16),
            sm((2, 16), i32),
            sm((1, 4), i32),
            VM((4, 2, VB, 2048), BF16),
            VM((4, 2, VB, 256), F32),
            VM((4, 2, 2, 4 * VB, 128), F32),
            VM((2, 128, 256), F32),
            VM((2, 4, 8, 128, 256), BF16),
            VM((2, 4, 8, 32, 128), F32),
            VM((3, 8, 32, 128), F32),
            VM((4, 8, 32, 128), F32),
            VM((2, 4, 32, 128), F32),
            VM((2, 8, 32, 128), F32),
            VM((2, 128, 512), BF16),
            VM((2, 2, 32, 128), F32),
            VM((16, 2, 128, 256), BF16),
            VM((16, 2, 32, 128), F32),
            VM((16, 2, 8, 128), F32),
            VM((4, 8, 128), F32),
            VM((4, 8, 128), F32),
            dma((8,)),
            dma((8,)),
            dma((14,)),
            dma((4, 2)),
            dma((2,)),
            dma((6,)),
            dma((6,)),
            dma((2,)),
            dma((2,)),
            dma((4,)),
            dma((4,)),
            dma((3,)),
            dma((3,)),
        ],
        compiler_params=pltpu.CompilerParams(collective_id=0, has_side_effects=True, vmem_limit_bytes=56 << 20),
    )(
        image,
        beams,
        offsets.reshape(512, 2).T,
        stations.T,
        uv,
        observed,
        live.T,
        jnp.asarray(perm, BF16),
    )


def solution(mesh):
    finer = Mesh(
        mesh.devices.reshape(mesh.shape["stn"], 2, 2, 4, 2),
        ("stn", "chan_0", "chan_1", "tile_0", "tile_1"),
    )
    placed = (
        P(TILE, "stn", None),
        P(),
        P(CHAN, None, None),
        P(STN_TILE, None),
        P(None, STN_TILE, CHAN),
        P(None, STN_TILE, CHAN, None),
        P(STN_TILE, CHAN),
    )
    return jax.shard_map(
        on_device,
        mesh=finer,
        in_specs=placed,
        out_specs=P(None, STN_TILE, CHAN, None),
        check_vma=False,
    )
```
